32 devices in a mesh: dp: 1 (over z), tp: 32 (over x, y, core).
Axes of the slice: x: 4, y: 4, z: 1, core: 2. Of those that a mesh axis runs over, the one named last changes fastest.
The devices are a block of a 4x4x8 slice.
Arguments:
- x: bfloat16 [7168, 5120], P(('dp', 'tp'))
- w_gate: bfloat16 [5120, 16384], P(None, 'tp')
- w_up: bfloat16 [5120, 16384], P(None, 'tp')
- w_down: bfloat16 [16384, 5120], P('tp')
Outputs:
- output: bfloat16 [7168, 5120], P(('dp', 'tp'))
All inputs are finite; a program needn't handle non-finite values.
Results may differ from the reference program's by a relative error of at most 0.016.
Values are sent between devices in bfloat16 or wider.
A program may use at most 768 MiB of HBM per device.

```python
import jax
import jax.numpy as jnp

ROWS = 7168
D = 5120
FF = 16384


def setup_inputs(seed: int = 0, part: int = 0) -> dict:
    kx, kg, ku, kd = jax.random.split(jax.random.key(seed), 4)
    drawn = {
        "x": jax.random.normal(jax.random.fold_in(kx, part), (ROWS, D), jnp.float32),
        "w_gate": jax.random.normal(kg, (D, FF), jnp.float32) * D**-0.5,
        "w_up": jax.random.normal(ku, (D, FF), jnp.float32) * D**-0.5,
        "w_down": jax.random.normal(kd, (FF, D), jnp.float32) * FF**-0.5,
    }
    return {k: v.astype(jnp.bfloat16) for k, v in drawn.items()}


def reference(x, w_gate, w_up, w_down):
    gate = jnp.dot(x, w_gate, preferred_element_type=jnp.float32)
    up = jnp.dot(x, w_up, preferred_element_type=jnp.float32)
    hidden = (jax.nn.silu(gate) * up).astype(jnp.bfloat16)
    return jnp.dot(hidden, w_down, preferred_element_type=jnp.float32).astype(jnp.bfloat16)
```

```python
import functools
import math

import jax
import jax.numpy as jnp
from jax import lax
from jax.experimental import pallas as pl
from jax.experimental.pallas import tpu as pltpu
from jax.sharding import PartitionSpec as P

MESH = pl.DeviceIdType.MESH
F32, BF16 = jnp.float32, jnp.bfloat16
TU = 128
CW = 256


def kernel(side, x_ref, wg_ref, wu_ref, wd_ref, y_ref, G, U, D,
           xa, hid, rf, rn, rx, gt, wt, sf, sn, sx, own, yo,
           ssem, rsem, lsem, gsem, wsem, fs, fr, ns, nr, xs, xr, ysem):
    t = lax.axis_index("tp")
    core, row, col = t % 2, (t // 2) % side, t // (2 * side)

    def peer(dx, dy, dc):
        return (((col + dx + side) % side) * side + (row + dy + side) % side) * 2 + (core + dc) % 2

    XP, XM, X2 = peer(1, 0, 0), peer(-1, 0, 0), peer(2, 0, 0)
    YP, YM, CC = peer(0, 1, 0), peer(0, -1, 0), peer(0, 0, 1)

    R, d = x_ref.shape
    h = R // 2
    units = wg_ref.shape[1]
    k = units // 2
    NJ = d // CW

    barrier = pltpu.get_barrier_semaphore()
    for p in (XP, XM, X2, YP, YM, CC):
        pl.semaphore_signal(barrier, inc=1, device_id={"tp": p}, device_id_type=MESH)
    pl.semaphore_wait(barrier, 6)

    def remote(src, dst, s, r, to):
        return pltpu.make_async_remote_copy(
            src_ref=src, dst_ref=dst, send_sem=s, recv_sem=r, device_id={"tp": to}, device_id_type=MESH)

    jobs = {}

    def job(name, src, dst, to):
        i = len(jobs)
        jobs[name] = remote(src, dst, ssem.at[i], rsem.at[i], to)

    job("ax", x_ref, xa.at[0, pl.ds(R, R)], X2)
    job("r1", x_ref, xa.at[1, pl.ds(0, R)], YP)
    job("l1", x_ref, xa.at[2, pl.ds(0, R)], YM)
    job("r1x", xa.at[0, pl.ds(R, R)], xa.at[1, pl.ds(R, R)], YP)
    job("l1x", xa.at[0, pl.ds(R, R)], xa.at[2, pl.ds(R, R)], YM)
    job("d2p", xa.at[1, pl.ds(0, h)], xa.at[3, pl.ds(0, h)], YP)
    job("d2m", xa.at[2, pl.ds(h, h)], xa.at[3, pl.ds(h, h)], YM)
    job("d2xp", xa.at[1, pl.ds(R, h)], xa.at[3, pl.ds(R, h)], YP)
    job("d2xm", xa.at[2, pl.ds(R + h, h)], xa.at[3, pl.ds(R + h, h)], YM)
    job("mg", wg_ref, G.at[0], CC)
    job("mu", wu_ref, U.at[0], CC)
    job("md", wd_ref, D.at[0], CC)
    for i, to in ((0, XP), (1, XM)):
        lo = pl.ds(i * k, k)
        job(f"ng{i}", wg_ref.at[:, lo], G.at[1, :, lo], to)
        job(f"nu{i}", wu_ref.at[:, lo], U.at[1, :, lo], to)
        for q in range(2):
            rows = pl.ds(i * k + q * (k // 2), k // 2)
            job(f"nd{i}{q}", wd_ref.at[rows], D.at[1, rows], to)
            job(f"qd{i}{q}", D.at[1, rows], D.at[2, rows], CC)
        job(f"qg{i}", G.at[1, :, lo], G.at[2, :, lo], CC)
        job(f"qu{i}", U.at[1, :, lo], U.at[2, :, lo], CC)

    def start(*names):
        for a in names:
            jobs[a].start()

    def got(*names):
        for a in names:
            jobs[a].wait_recv()

    mine = pltpu.make_async_copy(x_ref, xa.at[0, pl.ds(0, R)], lsem)
    mine.start()
    start("ax", "r1", "l1", "mg", "mu")
    start("ng0", "ng1", "nu0", "nu1", "nd00", "nd10", "nd01", "nd11", "md")

    per = units // TU

    def tile(tt, slot, act):
        kind = tt // per
        cols = pl.ds(pl.multiple_of((tt % per) * TU, TU), TU)
        for i, (w, b) in enumerate(((wg_ref, G), (wu_ref, U))):
            dst = gt.at[slot, :, pl.ds(i * TU, TU)]
            if act == "wait":
                pltpu.make_async_copy(w.at[:, pl.ds(0, TU)], dst, gsem.at[slot, i]).wait()
                continue

            @pl.when(kind == 0)
            def _():
                pltpu.make_async_copy(w.at[:, cols], dst, gsem.at[slot, i]).start()

            @pl.when(kind > 0)
            def _():
                pltpu.make_async_copy(b.at[jnp.maximum(kind - 1, 0), :, cols], dst, gsem.at[slot, i]).start()

    def hidden(t0, nt, g0, g1):
        tile(t0, 0, "start")

        def body(i, _):
            slot = i % 2

            @pl.when(i + 1 < nt)
            def _():
                tile(t0 + i + 1, 1 - slot, "start")

            tile(t0 + i, slot, "wait")

            def group(g, _):
                acc = jnp.dot(xa[g], gt[slot], preferred_element_type=F32)
                cols = pl.ds(pl.multiple_of((t0 + i) * TU, TU), TU)
                hid[g, :, cols] = (jax.nn.silu(acc[:, :TU]) * acc[:, TU:]).astype(BF16)
                return 0

            lax.fori_loop(g0, g1, group, 0)
            return 0

        lax.fori_loop(0, nt, body, 0)

    got("ax")
    start("r1x", "l1x")
    got("r1")
    start("d2p")
    got("l1")
    start("d2m")
    got("r1x")
    start("d2xp")
    got("l1x")
    start("d2xm")
    mine.wait()
    got("mg", "mu")
    hidden(0, 2 * per, 0, 3)
    got("ng0", "ng1")
    start("qg0", "qg1")
    got("d2p", "d2m", "d2xp", "d2xm")
    hidden(0, 2 * per, 3, 4)
    got("nu0", "nu1")
    start("qu0", "qu1")
    got("qg0", "qg1", "qu0", "qu1")
    hidden(2 * per, 2 * per, 0, 4)
    got("nd00", "nd10")
    start("qd00", "qd10")
    got("nd01", "nd11")
    start("qd01", "qd11")
    got("md", "qd00", "qd10", "qd01", "qd11")

    def wtile(s, j, act):
        slot = j % 2
        cols = pl.ds(pl.multiple_of(j * CW, CW), CW)
        for i in range(4):
            src = wd_ref.at[:, cols] if i == 0 else D.at[i - 1, :, cols]
            c = pltpu.make_async_copy(src, wt.at[s, slot, pl.ds(i * units, units)], wsem.at[s, slot, i])
            c.start() if act == "start" else c.wait()

    for s in range(3):
        wtile(s, 0, "start")

    def term(s, g, j):
        @pl.when(j + 1 < NJ)
        def _():
            wtile(s, j + 1, "start")

        wtile(s, j, "wait")

    def far(j, i):
        to = YP if i == 0 else YM
        return remote(sf.at[j % 2, i], rf.at[i, j], fs.at[j % 2, i], fr.at[i, j], to)

    def near(j, i):
        to = YP if i == 0 else YM
        return remote(sn.at[j % 2, i], rn.at[i, j], ns.at[j % 2, i], nr.at[i, j], to)

    def across(j):
        return remote(sx.at[j % 2], rx.at[j], xs.at[j % 2], xr.at[j], X2)

    def store(j):
        cols = pl.ds(pl.multiple_of(j * CW, CW), CW)
        return pltpu.make_async_copy(yo.at[j % 2], y_ref.at[:, cols], ysem.at[j % 2])

    def step(i, _):
        @pl.when(i < NJ)
        def _():
            j = i
            slot = j % 2
            term(0, 3, j)
            acc = jnp.dot(hid[3], wt[0, slot], preferred_element_type=F32).astype(BF16)

            @pl.when(j >= 2)
            def _():
                far(j - 2, 0).wait_send()
                far(j - 2, 1).wait_send()

            for a in range(2):
                for b in range(2):
                    sf[slot, a, b] = acc[b * R + a * h:b * R + (a + 1) * h]
            far(j, 0).start()
            far(j, 1).start()

        @pl.when(jnp.logical_and(i >= 1, i < NJ + 1))
        def _():
            j = i - 1
            slot = j % 2
            term(1, 1, j)
            a2 = jnp.dot(hid[2], wt[1, slot], preferred_element_type=F32)
            a1 = jnp.dot(hid[1], wt[1, slot], preferred_element_type=F32)

            @pl.when(j >= 2)
            def _():
                near(j - 2, 0).wait_send()
                near(j - 2, 1).wait_send()

            far(j, 0).wait_recv()
            for b in range(2):
                sn[slot, 0, b * R:b * R + h] = (a2[b * R:b * R + h] + rf[0, j, b].astype(F32)).astype(BF16)
                sn[slot, 0, b * R + h:(b + 1) * R] = a2[b * R + h:(b + 1) * R].astype(BF16)
            near(j, 0).start()
            far(j, 1).wait_recv()
            for b in range(2):
                sn[slot, 1, b * R:b * R + h] = a1[b * R:b * R + h].astype(BF16)
                sn[slot, 1, b * R + h:(b + 1) * R] = (a1[b * R + h:(b + 1) * R] + rf[1, j, b].astype(F32)).astype(BF16)
            near(j, 1).start()

        @pl.when(jnp.logical_and(i >= 2, i < NJ + 2))
        def _():
            j = i - 2
            slot = j % 2
            term(2, 0, j)
            acc = jnp.dot(hid[0], wt[2, slot], preferred_element_type=F32)

            @pl.when(j >= 2)
            def _():
                across(j - 2).wait_send()

            near(j, 0).wait_recv()
            near(j, 1).wait_recv()
            acc = acc + rn[0, j].astype(F32) + rn[1, j].astype(F32)
            own[slot] = acc[:R]
            sx[slot] = acc[R:].astype(BF16)
            across(j).start()

        @pl.when(i >= 3)
        def _():
            j = i - 3
            slot = j % 2

            @pl.when(j >= 2)
            def _():
                store(j - 2).wait()

            across(j).wait_recv()
            yo[slot] = (own[slot] + rx[j].astype(F32)).astype(BF16)
            store(j).start()

        return 0

    lax.fori_loop(0, NJ + 3, step, 0)
    for j in (NJ - 2, NJ - 1):
        for i in range(2):
            far(j, i).wait_send()
            near(j, i).wait_send()
        across(j).wait_send()
        store(j).wait()
    for a in jobs.values():
        a.wait_send()


def solution(mesh):
    side = math.isqrt(mesh.shape["tp"] // 2)

    def step(x, wg, wu, wd):
        R, d = x.shape
        h = R // 2
        units = wg.shape[1]
        NJ = d // CW
        hbm = pl.BlockSpec(memory_space=pltpu.HBM)
        dma = pltpu.SemaphoreType.DMA
        n_jobs = 28
        out = pl.pallas_call(
            functools.partial(kernel, side),
            name="mlp_ring",
            out_shape=[
                jax.ShapeDtypeStruct((R, d), BF16),
                jax.ShapeDtypeStruct((3, d, units), BF16),
                jax.ShapeDtypeStruct((3, d, units), BF16),
                jax.ShapeDtypeStruct((3, units, d), BF16),
            ],
            in_specs=[hbm] * 4,
            out_specs=[hbm] * 4,
            scratch_shapes=[
                pltpu.VMEM((4, 2 * R, d), BF16),
                pltpu.VMEM((4, 2 * R, 4 * units), BF16),
                pltpu.VMEM((2, NJ, 2, h, CW), BF16),
                pltpu.VMEM((2, NJ, 2 * R, CW), BF16),
                pltpu.VMEM((NJ, R, CW), BF16),
                pltpu.VMEM((2, d, 2 * TU), BF16),
                pltpu.VMEM((3, 2, 4 * units, CW), BF16),
                pltpu.VMEM((2, 2, 2, h, CW), BF16),
                pltpu.VMEM((2, 2, 2 * R, CW), BF16),
                pltpu.VMEM((2, R, CW), BF16),
                pltpu.VMEM((2, R, CW), F32),
                pltpu.VMEM((2, R, CW), BF16),
                dma((n_jobs,)), dma((n_jobs,)), dma, dma((2, 2)), dma((3, 2, 4)),
                dma((2, 2)), dma((2, NJ)), dma((2, 2)), dma((2, NJ)), dma((2,)), dma((NJ,)), dma((2,)),
            ],
            compiler_params=pltpu.CompilerParams(
                collective_id=0, has_side_effects=True, vmem_limit_bytes=67043328),
        )(x, wg, wu, wd)
        return out[0]

    return jax.shard_map(
        step,
        mesh=mesh,
        in_specs=(P(("dp", "tp"), None), P(None, "tp"), P(None, "tp"), P("tp", None)),
        out_specs=P(("dp", "tp"), None),
        check_vma=False,
    )
```

```python
import functools
import math

import jax
import jax.numpy as jnp
from jax import lax
from jax.experimental import pallas as pl
from jax.experimental.pallas import tpu as pltpu
from jax.sharding import PartitionSpec as P

MESH = pl.DeviceIdType.MESH
F32, BF16 = jnp.float32, jnp.bfloat16
TU = 128
CW = 256
AHEAD = 6
LAG = (5, 7, 10)
SLOTS = 4


def kernel(side, x_ref, wg_ref, wu_ref, wd_ref, y_ref, G, U, D,
           xa, hid, rf, rn, rx, gt, wt, sf, sn, sx, own, yo,
           ssem, rsem, lsem, gsem, wsem, fs, fr, ns, nr, xs, xr, ysem, ds, dr, qs, qr):
    t = lax.axis_index("tp")
    core, row, col = t % 2, (t // 2) % side, t // (2 * side)

    def peer(dx, dy, dc):
        return (((col + dx + side) % side) * side + (row + dy + side) % side) * 2 + (core + dc) % 2

    XP, XM, X2 = peer(1, 0, 0), peer(-1, 0, 0), peer(2, 0, 0)
    YP, YM, CC = peer(0, 1, 0), peer(0, -1, 0), peer(0, 0, 1)

    R, d = x_ref.shape
    h = R // 2
    units = wg_ref.shape[1]
    k = units // 2
    NJ = d // CW

    barrier = pltpu.get_barrier_semaphore()
    for p in (XP, XM, X2, YP, YM, CC):
        pl.semaphore_signal(barrier, inc=1, device_id={"tp": p}, device_id_type=MESH)
    pl.semaphore_wait(barrier, 6)

    def remote(src, dst, s, r, to):
        return pltpu.make_async_remote_copy(
            src_ref=src, dst_ref=dst, send_sem=s, recv_sem=r, device_id={"tp": to}, device_id_type=MESH)

    jobs = {}

    def job(name, src, dst, to):
        i = len(jobs)
        jobs[name] = remote(src, dst, ssem.at[i], rsem.at[i], to)

    job("ax", x_ref, xa.at[0, pl.ds(R, R)], X2)
    job("r1", x_ref, xa.at[1, pl.ds(0, R)], YP)
    job("l1", x_ref, xa.at[2, pl.ds(0, R)], YM)
    job("r1x", xa.at[0, pl.ds(R, R)], xa.at[1, pl.ds(R, R)], YP)
    job("l1x", xa.at[0, pl.ds(R, R)], xa.at[2, pl.ds(R, R)], YM)
    job("d2p", xa.at[1, pl.ds(0, h)], xa.at[3, pl.ds(0, h)], YP)
    job("d2m", xa.at[2, pl.ds(h, h)], xa.at[3, pl.ds(h, h)], YM)
    job("d2xp", xa.at[1, pl.ds(R, h)], xa.at[3, pl.ds(R, h)], YP)
    job("d2xm", xa.at[2, pl.ds(R + h, h)], xa.at[3, pl.ds(R + h, h)], YM)
    job("mg", wg_ref, G.at[0], CC)
    job("mu", wu_ref, U.at[0], CC)
    job("md", wd_ref, D.at[0], CC)
    for i, to in ((0, XP), (1, XM)):
        for q in range(2):
            lo = pl.ds(i * k + q * TU, TU)
            job(f"ng{i}{q}", wg_ref.at[:, lo], G.at[1, :, lo], to)
            job(f"nu{i}{q}", wu_ref.at[:, lo], U.at[1, :, lo], to)
            job(f"qg{i}{q}", G.at[1, :, lo], G.at[2, :, lo], CC)
            job(f"qu{i}{q}", U.at[1, :, lo], U.at[2, :, lo], CC)

    def columns(j):
        return pl.ds(pl.multiple_of(j * CW, CW), CW)

    def down(j, i):
        rows = pl.ds(i * k, k)
        return remote(wd_ref.at[rows, columns(j)], D.at[1, rows, columns(j)], ds.at[j, i], dr.at[j, i], XM if i else XP)

    def pass_on(j):
        return remote(D.at[1, :, columns(j)], D.at[2, :, columns(j)], qs.at[j], qr.at[j], CC)

    def start(*names):
        for a in names:
            jobs[a].start()

    def got(*names):
        for a in names:
            jobs[a].wait_recv()

    mine = pltpu.make_async_copy(x_ref, xa.at[0, pl.ds(0, R)], lsem)
    mine.start()
    start("ax", "r1", "l1", "mg", "mu")
    for q in range(2):
        start(f"ng0{q}", f"ng1{q}", f"nu0{q}", f"nu1{q}")
    start("md")
    for j in range(AHEAD):
        down(j, 0).start()
        down(j, 1).start()

    per = units // TU

    def tile(tt, slot, act):
        kind = tt // per
        cols = pl.ds(pl.multiple_of((tt % per) * TU, TU), TU)
        for i, (w, b) in enumerate(((wg_ref, G), (wu_ref, U))):
            dst = gt.at[slot, :, pl.ds(i * TU, TU)]
            if act == "wait":
                pltpu.make_async_copy(w.at[:, pl.ds(0, TU)], dst, gsem.at[slot, i]).wait()
                continue

            @pl.when(kind == 0)
            def _():
                pltpu.make_async_copy(w.at[:, cols], dst, gsem.at[slot, i]).start()

            @pl.when(kind > 0)
            def _():
                pltpu.make_async_copy(b.at[jnp.maximum(kind - 1, 0), :, cols], dst, gsem.at[slot, i]).start()

    def hidden(t0, by, nt, g0, g1, first=True, then=None):
        if first:
            tile(t0, 0, "start")

        def body(i, _):
            slot = i % 2
            if then is None:
                @pl.when(i + 1 < nt)
                def _():
                    tile(t0 + (i + 1) * by, 1 - slot, "start")
            else:
                tile(jnp.where(i + 1 < nt, t0 + (i + 1) * by, then), 1 - slot, "start")

            tile(t0, slot, "wait")

            def group(g, _):
                acc = jnp.dot(xa[g], gt[slot], preferred_element_type=F32)
                cols = pl.ds(pl.multiple_of((t0 + i * by) * TU, TU), TU)
                hid[g, :, cols] = (jax.nn.silu(acc[:, :TU]) * acc[:, TU:]).astype(BF16)
                return 0

            lax.fori_loop(g0, g1, group, 0)
            return 0

        lax.fori_loop(0, nt, body, 0)

    def swapped(act, q):
        for a in ("g", "u"):
            for i in range(2):
                if act == "take":
                    got(f"n{a}{i}{q}")
                    start(f"q{a}{i}{q}")
                else:
                    got(f"q{a}{i}{q}")

    nb = 2 * per
    got("ax")
    start("r1x", "l1x")
    got("r1")
    start("d2p")
    got("l1")
    start("d2m")
    mine.wait()
    got("mg", "mu")
    hidden(0, 1, nb, 0, 1, then=0)
    got("r1x")
    start("d2xp")
    got("l1x")
    start("d2xm")
    swapped("take", 0)
    hidden(0, 1, nb, 1, 3, first=False, then=nb)
    swapped("wait", 0)
    hidden(nb, 2, per, 0, 3, first=False, then=0)
    got("d2p", "d2m", "d2xp", "d2xm")
    hidden(0, 1, nb, 3, 4, first=False, then=nb)
    hidden(nb, 2, per, 3, 4, first=False)
    swapped("take", 1)
    hidden(nb + 1, 2, per // 2, 3, 4, then=nb + 1)
    hidden(nb + 1, 2, per // 2, 1, 3, first=False)
    swapped("wait", 1)
    hidden(nb + 1 + per, 2, per // 2, 3, 4, then=nb + 1 + per)

    def wtile(s, j, act):
        slot = j % 2
        cols = pl.ds(pl.multiple_of(j * CW, CW), CW)
        for i in range(4):
            src = wd_ref.at[:, cols] if i == 0 else D.at[i - 1, :, cols]
            c = pltpu.make_async_copy(src, wt.at[s, slot, pl.ds(i * units, units)], wsem.at[s, slot, i])
            c.start() if act == "start" else c.wait()

    def take_down(j):
        down(j, 0).wait_recv()
        down(j, 1).wait_recv()
        pass_on(j).start()

    def term(s, j):
        wtile(s, j, "wait")

        @pl.when(j + 1 < NJ)
        def _():
            wtile(s, j + 1, "start")

    def far(j, i):
        to = YP if i == 0 else YM
        return remote(sf.at[j % SLOTS, i], rf.at[i, j], fs.at[j % SLOTS, i], fr.at[i, j], to)

    def near(j, i):
        to = YP if i == 0 else YM
        return remote(sn.at[j % SLOTS, i], rn.at[i, j], ns.at[j % SLOTS, i], nr.at[i, j], to)

    def across(j):
        return remote(sx.at[j % SLOTS], rx.at[j], xs.at[j % SLOTS], xr.at[j], X2)

    def store(j):
        cols = pl.ds(pl.multiple_of(j * CW, CW), CW)
        return pltpu.make_async_copy(yo.at[j % 2], y_ref.at[:, cols], ysem.at[j % 2])

    def far_step(j):
        slot = j % SLOTS
        wtile(0, j, "wait")
        acc = jnp.dot(hid[3], wt[0, j % 2], preferred_element_type=F32).astype(BF16)

        @pl.when(j >= SLOTS)
        def _():
            far(j - SLOTS, 0).wait_send()
            far(j - SLOTS, 1).wait_send()

        for a in range(2):
            for b in range(2):
                sf[slot, a, b] = acc[b * R + a * h:b * R + (a + 1) * h]
        far(j, 0).start()
        far(j, 1).start()

        @pl.when(j + 1 < NJ)
        def _():
            pass_on(j + 1).wait_recv()
            wtile(0, j + 1, "start")

        @pl.when(j + 2 < NJ)
        def _():
            take_down(j + 2)

        @pl.when(j + AHEAD < NJ)
        def _():
            down(j + AHEAD, 0).start()
            down(j + AHEAD, 1).start()

    def near_step(j):
        slot = j % SLOTS
        term(1, j)
        a2 = jnp.dot(hid[2], wt[1, j % 2], preferred_element_type=F32)
        a1 = jnp.dot(hid[1], wt[1, j % 2], preferred_element_type=F32)

        @pl.when(j >= SLOTS)
        def _():
            near(j - SLOTS, 0).wait_send()
            near(j - SLOTS, 1).wait_send()

        far(j, 0).wait_recv()
        for b in range(2):
            sn[slot, 0, b * R:b * R + h] = (a2[b * R:b * R + h] + rf[0, j, b].astype(F32)).astype(BF16)
            sn[slot, 0, b * R + h:(b + 1) * R] = a2[b * R + h:(b + 1) * R].astype(BF16)
        near(j, 0).start()
        far(j, 1).wait_recv()
        for b in range(2):
            sn[slot, 1, b * R:b * R + h] = a1[b * R:b * R + h].astype(BF16)
            sn[slot, 1, b * R + h:(b + 1) * R] = (a1[b * R + h:(b + 1) * R] + rf[1, j, b].astype(F32)).astype(BF16)
        near(j, 1).start()

    def own_step(j):
        slot = j % SLOTS
        term(2, j)
        acc = jnp.dot(hid[0], wt[2, j % 2], preferred_element_type=F32)

        @pl.when(j >= SLOTS)
        def _():
            across(j - SLOTS).wait_send()

        near(j, 0).wait_recv()
        near(j, 1).wait_recv()
        acc = acc + rn[0, j].astype(F32) + rn[1, j].astype(F32)
        own[slot] = acc[:R]
        sx[slot] = acc[R:].astype(BF16)
        across(j).start()

    def last_step(j):
        @pl.when(j >= 2)
        def _():
            store(j - 2).wait()

        across(j).wait_recv()
        yo[j % 2] = (own[j % SLOTS] + rx[j].astype(F32)).astype(BF16)
        store(j).start()

    def loop(lo, hi, f):
        def body(i, _):
            f(i)
            return 0

        lax.fori_loop(lo, hi, body, 0)

    got("md")
    take_down(0)
    pass_on(0).wait_recv()
    for s in range(3):
        wtile(s, 0, "start")
    take_down(1)
    loop(0, 2, far_step)
    hidden(nb + 1 + per, 2, per // 2, 1, 3, first=False, then=nb + 1)
    loop(2, LAG[0], far_step)
    hidden(nb + 1, 2, per, 0, 1, first=False)

    def step(i):
        @pl.when(i < NJ)
        def _():
            far_step(i)

        @pl.when(i < NJ + LAG[0])
        def _():
            near_step(i - LAG[0])

        @pl.when(jnp.logical_and(i >= LAG[1], i < NJ + LAG[1]))
        def _():
            own_step(i - LAG[1])

        @pl.when(i >= LAG[2])
        def _():
            last_step(i - LAG[2])

    loop(LAG[0], NJ + LAG[2], step)
    for j in range(NJ - SLOTS, NJ):
        for i in range(2):
            far(j, i).wait_send()
            near(j, i).wait_send()
        across(j).wait_send()
    store(NJ - 2).wait()
    store(NJ - 1).wait()

    def sent(j):
        down(j, 0).wait_send()
        down(j, 1).wait_send()
        pass_on(j).wait_send()

    loop(0, NJ, sent)
    for a in jobs.values():
        a.wait_send()


def solution(mesh):
    side = math.isqrt(mesh.shape["tp"] // 2)

    def step(x, wg, wu, wd):
        R, d = x.shape
        h = R // 2
        units = wg.shape[1]
        NJ = d // CW
        hbm = pl.BlockSpec(memory_space=pltpu.HBM)
        dma = pltpu.SemaphoreType.DMA
        n_jobs = 28
        out = pl.pallas_call(
            functools.partial(kernel, side),
            name="mlp_ring",
            out_shape=[
                jax.ShapeDtypeStruct((R, d), BF16),
                jax.ShapeDtypeStruct((3, d, units), BF16),
                jax.ShapeDtypeStruct((3, d, units), BF16),
                jax.ShapeDtypeStruct((3, units, d), BF16),
            ],
            in_specs=[hbm] * 4,
            out_specs=[hbm] * 4,
            scratch_shapes=[
                pltpu.VMEM((4, 2 * R, d), BF16),
                pltpu.VMEM((4, 2 * R, 4 * units), BF16),
                pltpu.VMEM((2, NJ, 2, h, CW), BF16),
                pltpu.VMEM((2, NJ, 2 * R, CW), BF16),
                pltpu.VMEM((NJ, R, CW), BF16),
                pltpu.VMEM((2, d, 2 * TU), BF16),
                pltpu.VMEM((3, 2, 4 * units, CW), BF16),
                pltpu.VMEM((SLOTS, 2, 2, h, CW), BF16),
                pltpu.VMEM((SLOTS, 2, 2 * R, CW), BF16),
                pltpu.VMEM((SLOTS, R, CW), BF16),
                pltpu.VMEM((SLOTS, R, CW), F32),
                pltpu.VMEM((2, R, CW), BF16),
                dma((n_jobs,)), dma((n_jobs,)), dma, dma((2, 2)), dma((3, 2, 4)),
                dma((SLOTS, 2)), dma((2, NJ)), dma((SLOTS, 2)), dma((2, NJ)), dma((SLOTS,)), dma((NJ,)), dma((2,)),
                dma((NJ, 2)), dma((NJ, 2)), dma((NJ,)), dma((NJ,)),
            ],
            compiler_params=pltpu.CompilerParams(
                collective_id=0, has_side_effects=True, vmem_limit_bytes=67043328),
        )(x, wg, wu, wd)
        return out[0]

    return jax.shard_map(
        step,
        mesh=mesh,
        in_specs=(P(("dp", "tp"), None), P(None, "tp"), P(None, "tp"), P("tp", None)),
        out_specs=P(("dp", "tp"), None),
        check_vma=False,
    )
```

```python
import functools
import math

import jax
import jax.numpy as jnp
from jax import lax
from jax.experimental import pallas as pl
from jax.experimental.pallas import tpu as pltpu
from jax.sharding import PartitionSpec as P

MESH = pl.DeviceIdType.MESH
F32, BF16 = jnp.float32, jnp.bfloat16
TU = 128
CW = 256
AHEAD = 9
LAG = (5, 7, 12)
SLOTS = 4
CROSS = 3
WIDE = 6


def kernel(side, x_ref, wg_ref, wu_ref, wd_ref, y_ref, G, U, D,
           xa, hid, rf, rn, rx, gt, wt, sf, sn, sx, own, yo,
           ssem, rsem, lsem, gsem, wsem, fs, fr, ns, nr, xs, xr, ysem, ds, dr, qs, qr,
           wx, so, ro, xsem, os, orr):
    t = lax.axis_index("tp")
    core, row, col = t % 2, (t // 2) % side, t // (2 * side)

    def peer(dx, dy, dc):
        return (((col + dx + side) % side) * side + (row + dy + side) % side) * 2 + (core + dc) % 2

    XP, XM, X2 = peer(1, 0, 0), peer(-1, 0, 0), peer(2, 0, 0)
    YP, YM, CC = peer(0, 1, 0), peer(0, -1, 0), peer(0, 0, 1)

    R, d = x_ref.shape
    h = R // 2
    units = wg_ref.shape[1]
    k = units // 2
    NJ = d // CW
    N0 = NJ - CROSS

    barrier = pltpu.get_barrier_semaphore()
    for p in (XP, XM, X2, YP, YM, CC):
        pl.semaphore_signal(barrier, inc=1, device_id={"tp": p}, device_id_type=MESH)
    pl.semaphore_wait(barrier, 6)

    def remote(src, dst, s, r, to):
        return pltpu.make_async_remote_copy(
            src_ref=src, dst_ref=dst, send_sem=s, recv_sem=r, device_id={"tp": to}, device_id_type=MESH)

    jobs = {}

    def job(name, src, dst, to):
        i = len(jobs)
        jobs[name] = remote(src, dst, ssem.at[i], rsem.at[i], to)

    job("ax", x_ref, xa.at[0, pl.ds(R, R)], X2)
    job("r1", x_ref, xa.at[1, pl.ds(0, R)], YP)
    job("l1", x_ref, xa.at[2, pl.ds(0, R)], YM)
    job("r1x", xa.at[0, pl.ds(R, R)], xa.at[1, pl.ds(R, R)], YP)
    job("l1x", xa.at[0, pl.ds(R, R)], xa.at[2, pl.ds(R, R)], YM)
    job("d2p", xa.at[1, pl.ds(0, h)], xa.at[3, pl.ds(0, h)], YP)
    job("d2m", xa.at[2, pl.ds(h, h)], xa.at[3, pl.ds(h, h)], YM)
    job("d2xp", xa.at[1, pl.ds(R, h)], xa.at[3, pl.ds(R, h)], YP)
    job("d2xm", xa.at[2, pl.ds(R + h, h)], xa.at[3, pl.ds(R + h, h)], YM)
    job("mg", wg_ref, G.at[0], CC)
    job("mu", wu_ref, U.at[0], CC)
    job("md", wd_ref, D.at[0], CC)
    for i, to in ((0, XP), (1, XM)):
        for q in range(2):
            lo = pl.ds(i * k + q * TU, TU)
            job(f"ng{i}{q}", wg_ref.at[:, lo], G.at[1, :, lo], to)
            job(f"nu{i}{q}", wu_ref.at[:, lo], U.at[1, :, lo], to)
            job(f"qg{i}{q}", G.at[1, :, lo], G.at[2, :, lo], CC)
            job(f"qu{i}{q}", U.at[1, :, lo], U.at[2, :, lo], CC)

    def columns(j):
        return pl.ds(pl.multiple_of(j * CW, CW), CW)

    def down(j, i):
        rows = pl.ds(i * k, k)
        return remote(wd_ref.at[rows, columns(j)], D.at[1, rows, columns(j)], ds.at[j, i], dr.at[j, i], XM if i else XP)

    def pass_on(j):
        return remote(D.at[1, :, columns(j)], D.at[2, :, columns(j)], qs.at[j], qr.at[j], CC)

    def start(*names):
        for a in names:
            jobs[a].start()

    def got(*names):
        for a in names:
            jobs[a].wait_recv()

    mine = pltpu.make_async_copy(x_ref, xa.at[0, pl.ds(0, R)], lsem)
    mine.start()
    start("ax", "r1", "l1", "mg", "mu")
    for q in range(2):
        start(f"ng0{q}", f"ng1{q}", f"nu0{q}", f"nu1{q}")
    start("md")
    for j in range(AHEAD):
        down(j, 0).start()
        down(j, 1).start()

    per = units // TU

    def tile(tt, slot, act):
        kind = tt // per
        cols = pl.ds(pl.multiple_of((tt % per) * TU, TU), TU)
        for i, (w, b) in enumerate(((wg_ref, G), (wu_ref, U))):
            dst = gt.at[slot, :, pl.ds(i * TU, TU)]
            if act == "wait":
                pltpu.make_async_copy(w.at[:, pl.ds(0, TU)], dst, gsem.at[slot, i]).wait()
                continue

            @pl.when(kind == 0)
            def _():
                pltpu.make_async_copy(w.at[:, cols], dst, gsem.at[slot, i]).start()

            @pl.when(kind > 0)
            def _():
                pltpu.make_async_copy(b.at[jnp.maximum(kind - 1, 0), :, cols], dst, gsem.at[slot, i]).start()

    def hidden(t0, by, nt, g0, g1, first=True, then=None):
        if first:
            tile(t0, 0, "start")

        def body(i, _):
            slot = i % 2
            if then is None:
                @pl.when(i + 1 < nt)
                def _():
                    tile(t0 + (i + 1) * by, 1 - slot, "start")
            else:
                tile(jnp.where(i + 1 < nt, t0 + (i + 1) * by, then), 1 - slot, "start")

            tile(t0, slot, "wait")

            def group(g, _):
                acc = jnp.dot(xa[g], gt[slot], preferred_element_type=F32)
                cols = pl.ds(pl.multiple_of((t0 + i * by) * TU, TU), TU)
                hid[g, :, cols] = (jax.nn.silu(acc[:, :TU]) * acc[:, TU:]).astype(BF16)
                return 0

            lax.fori_loop(g0, g1, group, 0)
            return 0

        lax.fori_loop(0, nt, body, 0)

    def swapped(act, q):
        for a in ("g", "u"):
            for i in range(2):
                if act == "take":
                    got(f"n{a}{i}{q}")
                    start(f"q{a}{i}{q}")
                else:
                    got(f"q{a}{i}{q}")

    nb = 2 * per
    got("ax")
    start("r1x", "l1x")
    got("r1")
    start("d2p")
    got("l1")
    start("d2m")
    mine.wait()
    got("mg", "mu")
    hidden(0, 1, nb, 0, 1, then=0)
    got("r1x")
    start("d2xp")
    got("l1x")
    start("d2xm")
    hidden(0, 1, nb, 1, 3, first=False)
    swapped("take", 0)
    hidden(nb, 2, per // 2, 0, 3)
    swapped("wait", 0)
    hidden(nb + per, 2, per // 2, 0, 3, then=0)
    got("ng01", "ng11")
    start("qg01", "qg11")
    got("d2p", "d2m", "d2xp", "d2xm")
    hidden(0, 1, nb, 3, 4, first=False, then=nb)
    hidden(nb, 2, per, 3, 4, first=False)
    got("nu01", "nu11")
    start("qu01", "qu11")
    hidden(nb + 1, 2, per // 2, 3, 4, then=nb + 1)
    hidden(nb + 1, 2, per // 2, 1, 3, first=False)
    swapped("wait", 1)
    hidden(nb + 1 + per, 2, per // 2, 3, 4, then=nb + 1 + per)

    def wtile(s, j, act):
        slot = j % 2
        cols = pl.ds(pl.multiple_of(j * CW, CW), CW)
        for i in range(4):
            src = wd_ref.at[:, cols] if i == 0 else D.at[i - 1, :, cols]
            c = pltpu.make_async_copy(src, wt.at[s, slot, pl.ds(i * units, units)], wsem.at[s, slot, i])
            c.start() if act == "start" else c.wait()

    def take_down(j):
        down(j, 0).wait_recv()
        down(j, 1).wait_recv()
        pass_on(j).start()

    def term(s, j):
        wtile(s, j, "wait")

        @pl.when(j + 1 < NJ)
        def _():
            wtile(s, j + 1, "start")

    def far(j, i, half=False):
        to = YP if i == 0 else YM
        a, b = (sf.at[j % SLOTS, i, 0], rf.at[i, j, 0]) if half else (sf.at[j % SLOTS, i], rf.at[i, j])
        return remote(a, b, fs.at[j % SLOTS, i], fr.at[i, j], to)

    def near(j, i, half=False):
        to = YP if i == 0 else YM
        a, b = sn.at[j % SLOTS, i], rn.at[i, j]
        if half:
            a, b = a.at[pl.ds(0, R)], b.at[pl.ds(0, R)]
        return remote(a, b, ns.at[j % SLOTS, i], nr.at[i, j], to)

    def settle(what, j):
        for half, these in ((False, j < N0), (True, j >= N0)):
            @pl.when(these)
            def _():
                what(j, 0, half).wait_send()
                what(j, 1, half).wait_send()

    def across(j):
        return remote(sx.at[j % WIDE], rx.at[j], xs.at[j % WIDE], xr.at[j], X2)

    def store(j):
        cols = pl.ds(pl.multiple_of(j * CW, CW), CW)
        return pltpu.make_async_copy(yo.at[j % 2], y_ref.at[:, cols], ysem.at[j % 2])

    def over(j):
        return remote(so.at[j % 2], ro.at[j - N0], os.at[j % 2], orr.at[j - N0], X2)

    def xtile(j, act):
        for i in range(4):
            src = wd_ref.at[:, columns(j)] if i == 0 else D.at[i - 1, :, columns(j)]
            c = pltpu.make_async_copy(src, wx.at[pl.ds(i * units, units)], xsem.at[i])
            c.start() if act == "start" else c.wait()

    def over_step(j):
        @pl.when(j >= N0 + 2)
        def _():
            over(j - 2).wait_send()

        xtile(j, "wait")

        def group(g, _):
            so[j % 2, g] = jnp.dot(hid[g, R:], wx[...], preferred_element_type=F32).astype(BF16)
            return 0

        lax.fori_loop(0, 4, group, 0)
        over(j).start()

    def far_step(j):
        slot = j % SLOTS
        wtile(0, j, "wait")

        @pl.when(j >= SLOTS)
        def _():
            settle(far, j - SLOTS)

        @pl.when(j < N0)
        def _():
            acc = jnp.dot(hid[3], wt[0, j % 2], preferred_element_type=F32).astype(BF16)
            for a in range(2):
                for b in range(2):
                    sf[slot, a, b] = acc[b * R + a * h:b * R + (a + 1) * h]
            far(j, 0).start()
            far(j, 1).start()

        @pl.when(j >= N0)
        def _():
            acc = jnp.dot(hid[3, :R], wt[0, j % 2], preferred_element_type=F32)
            over(j).wait_recv()
            acc = (acc + ro[jnp.maximum(j - N0, 0), 3].astype(F32)).astype(BF16)
            for a in range(2):
                sf[slot, a, 0] = acc[a * h:(a + 1) * h]
                far(j, a, True).start()

        @pl.when(j + 1 < N0)
        def _():
            pass_on(j + 1).wait_recv()

        @pl.when(j + 1 < NJ)
        def _():
            wtile(0, j + 1, "start")

        @pl.when(j + 2 < N0)
        def _():
            take_down(j + 2)

        @pl.when(j + AHEAD < N0)
        def _():
            down(j + AHEAD, 0).start()
            down(j + AHEAD, 1).start()

        @pl.when(j < NJ - N0)
        def _():
            down(j + N0, 0).start()
            down(j + N0, 1).start()

        @pl.when(jnp.logical_and(j % 2 == 0, jnp.logical_and(j >= 4, j < 4 + 2 * (NJ - N0))))
        def _():
            take_down(N0 + (j - 4) // 2)

    def near_step(j):
        slot = j % SLOTS
        term(1, j)
        @pl.when(j >= SLOTS)
        def _():
            settle(near, j - SLOTS)

        @pl.when(j < N0)
        def _():
            a2 = jnp.dot(hid[2], wt[1, j % 2], preferred_element_type=F32)
            a1 = jnp.dot(hid[1], wt[1, j % 2], preferred_element_type=F32)
            far(j, 0).wait_recv()
            for b in range(2):
                sn[slot, 0, b * R:b * R + h] = (a2[b * R:b * R + h] + rf[0, j, b].astype(F32)).astype(BF16)
                sn[slot, 0, b * R + h:(b + 1) * R] = a2[b * R + h:(b + 1) * R].astype(BF16)
            near(j, 0).start()
            far(j, 1).wait_recv()
            for b in range(2):
                sn[slot, 1, b * R:b * R + h] = a1[b * R:b * R + h].astype(BF16)
                sn[slot, 1, b * R + h:(b + 1) * R] = (a1[b * R + h:(b + 1) * R] + rf[1, j, b].astype(F32)).astype(BF16)
            near(j, 1).start()

        @pl.when(j >= N0)
        def _():
            o = jnp.maximum(j - N0, 0)
            a2 = jnp.dot(hid[2, :R], wt[1, j % 2], preferred_element_type=F32) + ro[o, 2].astype(F32)
            a1 = jnp.dot(hid[1, :R], wt[1, j % 2], preferred_element_type=F32) + ro[o, 1].astype(F32)
            far(j, 0, True).wait_recv()
            sn[slot, 0, :h] = (a2[:h] + rf[0, j, 0].astype(F32)).astype(BF16)
            sn[slot, 0, h:R] = a2[h:].astype(BF16)
            near(j, 0, True).start()
            far(j, 1, True).wait_recv()
            sn[slot, 1, :h] = a1[:h].astype(BF16)
            sn[slot, 1, h:R] = (a1[h:] + rf[1, j, 0].astype(F32)).astype(BF16)
            near(j, 1, True).start()

    def own_step(j):
        slot = j % WIDE
        term(2, j)

        @pl.when(j < N0)
        def _():
            acc = jnp.dot(hid[0], wt[2, j % 2], preferred_element_type=F32)

            @pl.when(j >= WIDE)
            def _():
                across(j - WIDE).wait_send()

            near(j, 0).wait_recv()
            near(j, 1).wait_recv()
            acc = acc + rn[0, j].astype(F32) + rn[1, j].astype(F32)
            own[slot] = acc[:R]
            sx[slot] = acc[R:].astype(BF16)
            across(j).start()

        @pl.when(j >= N0)
        def _():
            acc = jnp.dot(hid[0, :R], wt[2, j % 2], preferred_element_type=F32)
            acc = acc + ro[jnp.maximum(j - N0, 0), 0].astype(F32)
            near(j, 0, True).wait_recv()
            near(j, 1, True).wait_recv()
            own[slot] = acc + rn[0, j, :R].astype(F32) + rn[1, j, :R].astype(F32)

    def last_step(j):
        @pl.when(j >= 2)
        def _():
            store(j - 2).wait()

        @pl.when(j < N0)
        def _():
            across(j).wait_recv()
            yo[j % 2] = (own[j % WIDE] + rx[j].astype(F32)).astype(BF16)

        @pl.when(j >= N0)
        def _():
            yo[j % 2] = own[j % WIDE].astype(BF16)

        store(j).start()

    def loop(lo, hi, f):
        def body(i, _):
            f(i)
            return 0

        lax.fori_loop(lo, hi, body, 0)

    got("md")
    take_down(0)
    pass_on(0).wait_recv()
    for s in range(3):
        wtile(s, 0, "start")
    take_down(1)
    loop(0, 2, far_step)
    hidden(nb + 1 + per, 2, per // 2, 1, 3, first=False, then=nb + 1)
    loop(2, LAG[0], far_step)
    hidden(nb + 1, 2, per, 0, 1, first=False)

    def step(i):
        crossing = jnp.logical_and(i % 2 == 1, i < 5 + 2 * (NJ - N0))
        o = N0 + (i - 5) // 2

        @pl.when(crossing)
        def _():
            pass_on(o).wait_recv()
            xtile(o, "start")

        @pl.when(i < NJ)
        def _():
            far_step(i)

        @pl.when(i < NJ + LAG[0])
        def _():
            near_step(i - LAG[0])

        @pl.when(jnp.logical_and(i >= LAG[1], i < NJ + LAG[1]))
        def _():
            own_step(i - LAG[1])

        @pl.when(i >= LAG[2])
        def _():
            last_step(i - LAG[2])

        @pl.when(crossing)
        def _():
            over_step(o)

    loop(LAG[0], NJ + LAG[2], step)
    for j in range(NJ - SLOTS, NJ):
        for i in range(2):
            far(j, i, j >= N0).wait_send()
            near(j, i, j >= N0).wait_send()
    for j in range(N0 - WIDE, N0):
        across(j).wait_send()
    over(NJ - 2).wait_send()
    over(NJ - 1).wait_send()
    store(NJ - 2).wait()
    store(NJ - 1).wait()

    def sent(j):
        down(j, 0).wait_send()
        down(j, 1).wait_send()
        pass_on(j).wait_send()

    loop(0, NJ, sent)
    for a in jobs.values():
        a.wait_send()


def solution(mesh):
    side = math.isqrt(mesh.shape["tp"] // 2)

    def step(x, wg, wu, wd):
        R, d = x.shape
        h = R // 2
        units = wg.shape[1]
        NJ = d // CW
        hbm = pl.BlockSpec(memory_space=pltpu.HBM)
        dma = pltpu.SemaphoreType.DMA
        n_jobs = 28
        out = pl.pallas_call(
            functools.partial(kernel, side),
            name="mlp_ring",
            out_shape=[
                jax.ShapeDtypeStruct((R, d), BF16),
                jax.ShapeDtypeStruct((3, d, units), BF16),
                jax.ShapeDtypeStruct((3, d, units), BF16),
                jax.ShapeDtypeStruct((3, units, d), BF16),
            ],
            in_specs=[hbm] * 4,
            out_specs=[hbm] * 4,
            scratch_shapes=[
                pltpu.VMEM((4, 2 * R, d), BF16),
                pltpu.VMEM((4, 2 * R, 4 * units), BF16),
                pltpu.VMEM((2, NJ, 2, h, CW), BF16),
                pltpu.VMEM((2, NJ, 2 * R, CW), BF16),
                pltpu.VMEM((NJ, R, CW), BF16),
                pltpu.VMEM((2, d, 2 * TU), BF16),
                pltpu.VMEM((3, 2, 4 * units, CW), BF16),
                pltpu.VMEM((SLOTS, 2, 2, h, CW), BF16),
                pltpu.VMEM((SLOTS, 2, 2 * R, CW), BF16),
                pltpu.VMEM((WIDE, R, CW), BF16),
                pltpu.VMEM((WIDE, R, CW), F32),
                pltpu.VMEM((2, R, CW), BF16),
                dma((n_jobs,)), dma((n_jobs,)), dma, dma((2, 2)), dma((3, 2, 4)),
                dma((SLOTS, 2)), dma((2, NJ)), dma((SLOTS, 2)), dma((2, NJ)), dma((WIDE,)), dma((NJ,)), dma((2,)),
                dma((NJ, 2)), dma((NJ, 2)), dma((NJ,)), dma((NJ,)),
                pltpu.VMEM((4 * units, CW), BF16),
                pltpu.VMEM((2, 4, R, CW), BF16),
                pltpu.VMEM((CROSS, 4, R, CW), BF16),
                dma((4,)), dma((2,)), dma((CROSS,)),
            ],
            compiler_params=pltpu.CompilerParams(
                collective_id=0, has_side_effects=True, vmem_limit_bytes=67043328),
        )(x, wg, wu, wd)
        return out[0]

    return jax.shard_map(
        step,
        mesh=mesh,
        in_specs=(P(("dp", "tp"), None), P(None, "tp"), P(None, "tp"), P("tp", None)),
        out_specs=P(("dp", "tp"), None),
        check_vma=False,
    )
```
